32 devices in a mesh: seq: 32 (over z, y, x, core).
Axes of the slice: x: 2, y: 2, z: 4, core: 2. Of those that a mesh axis runs over, the one named last changes fastest.
Arguments:
- queries: bfloat16 [4096, 4096], P('seq'), may hold values from -48 to 48, as said below
- keys: bfloat16 [4096, 512], P('seq'), may hold values from -6 to 6, as said below
- values: bfloat16 [4096, 512], P('seq'), may hold values from -6 to 6
Outputs:
- attended: bfloat16 [4096, 4096], P('seq')
The draws below stay inside these ranges and needn't reach their ends.
Inputs may be any that keep to these rules, and one draw needn't show every extreme that they name: queries of every block, with 32 heads of 128 entries per token. keys of every block, with 4 heads of 128 entries per token.
All inputs are finite; a program needn't handle non-finite values.
Results may differ from the reference program's by a relative error of at most 0.0049.
Values may be sent and summed in bfloat16 or wider, within the bound.
A program may use at most 64 MiB of HBM per device.

```python
import math
import jax
import jax.numpy as jnp
from jax import lax

QUERY_HEADS = 32
KEY_VALUE_HEADS = 4
HEAD_SIZE = 128
BLOCK_TOKENS = 128
HALO = 64
CONTEXT_TOKENS = 4096
N_SEQ = 32


def shared_keys(key):
    source_tokens = jax.random.fold_in(key, 11)
    unscaled_scores = jnp.clip(jax.random.normal(source_tokens, (CONTEXT_TOKENS, KEY_VALUE_HEADS * HEAD_SIZE), jnp.float32), -6.0, 6.0)
    return unscaled_scores.astype(jnp.bfloat16)


def draw_keys(key, part):
    return shared_keys(key)


def draw_queries(key, part):
    source_tokens = jax.random.fold_in(key, 21)
    drawn = jnp.clip(jax.random.normal(source_tokens, (CONTEXT_TOKENS, QUERY_HEADS * HEAD_SIZE), jnp.float32), -6.0, 6.0)
    return drawn.astype(jnp.bfloat16)


def levels(own_key, dims, pieces, smallest, high):
    loudness = 1.0
    for dim, blocks in pieces:
        heights = jax.random.uniform(jax.random.fold_in(jax.random.fold_in(own_key, 6), dim), (blocks,), jnp.float32, smallest / len(pieces), high / len(pieces))
        loudness = loudness * jnp.repeat(jnp.exp(heights), dims[dim] // blocks).reshape((-1,) + (1,) * (len(dims) - 1 - dim))
    return loudness


def gaussian(own_key, shape, width, limit, cuts=(), held_as=jnp.bfloat16):
    factor_of = levels(own_key, shape, cuts, -0.22, 0.18) if cuts else 1.0
    drawn = jax.random.normal(own_key, shape, jnp.float32) * width * factor_of
    return jnp.minimum(jnp.maximum(drawn, -limit), limit).astype(held_as)


def setup_inputs(seed: int = 0) -> dict:
    seeds = jax.random.split(jax.random.key(seed), 4)
    queries = draw_queries(jax.random.fold_in(seeds[3], 71), 0)
    keys = draw_keys(jax.random.fold_in(seeds[3], 71), 0)
    values = gaussian(seeds[2], (CONTEXT_TOKENS, KEY_VALUE_HEADS * HEAD_SIZE), 1.0, 6.0, ((0, 32),))
    return {"queries": queries, "keys": keys, "values": values}


def reference(queries, keys, values):
    query_groups = QUERY_HEADS // KEY_VALUE_HEADS
    block_count = 2 * BLOCK_TOKENS + HALO
    scale = 1.0 / math.sqrt(HEAD_SIZE)
    anchor_keys = keys[:BLOCK_TOKENS]
    anchor_values = values[:BLOCK_TOKENS]
    row_ids = jnp.arange(BLOCK_TOKENS, dtype=jnp.int32)[:, None]
    col_ids = jnp.arange(BLOCK_TOKENS, dtype=jnp.int32)[None, :]

    def one_block(block):
        start = (block * BLOCK_TOKENS).astype(jnp.int32)
        halo_start = jnp.maximum(start - HALO, 0).astype(jnp.int32)
        query_matrix = lax.dynamic_slice_in_dim(queries, start, BLOCK_TOKENS, 0).astype(jnp.float32)
        query_matrix = query_matrix.reshape(BLOCK_TOKENS, KEY_VALUE_HEADS, query_groups, HEAD_SIZE)
        local_keys = lax.dynamic_slice_in_dim(keys, start, BLOCK_TOKENS, 0)
        local_values = lax.dynamic_slice_in_dim(values, start, BLOCK_TOKENS, 0)
        halo_keys = lax.dynamic_slice_in_dim(keys, halo_start, HALO, 0)
        halo_values = lax.dynamic_slice_in_dim(values, halo_start, HALO, 0)
        joined_keys = jnp.concatenate([anchor_keys, halo_keys, local_keys], axis=0).astype(jnp.float32).reshape(block_count, KEY_VALUE_HEADS, HEAD_SIZE)
        joined_values = jnp.concatenate([anchor_values, halo_values, local_values], axis=0).astype(jnp.float32).reshape(block_count, KEY_VALUE_HEADS, HEAD_SIZE)
        scores = jnp.einsum('thgd,khd->hgtk', query_matrix, joined_keys) * scale
        visible = jnp.concatenate([jnp.broadcast_to(block > 0, (BLOCK_TOKENS, BLOCK_TOKENS)), jnp.broadcast_to(block > 0, (BLOCK_TOKENS, HALO)), col_ids <= row_ids], axis=1)
        scores = jnp.where(visible, scores, jnp.float32(-1e+30))
        highest = lax.optimization_barrier(jnp.max(scores, axis=-1, keepdims=True))
        expo = jnp.exp(scores - highest)
        weights = (expo / lax.optimization_barrier(jnp.sum(expo, axis=-1, keepdims=True))).astype(jnp.bfloat16)
        mixed = jnp.einsum('hgtk,khd->thgd', weights.astype(jnp.float32), joined_values)
        return mixed.reshape(BLOCK_TOKENS, QUERY_HEADS * HEAD_SIZE).astype(jnp.bfloat16)
    blocks = lax.map(one_block, jnp.arange(N_SEQ, dtype=jnp.int32))
    return blocks.reshape(CONTEXT_TOKENS, QUERY_HEADS * HEAD_SIZE)
```

```python
import functools
import math

import jax
import jax.numpy as jnp
from jax import lax
from jax.experimental import pallas as pl
from jax.experimental.pallas import tpu as pltpu
from jax.sharding import PartitionSpec as P

KEY_VALUE_HEADS = 4
HEAD_SIZE = 128
HALO = 64
SUM_ROWS = 8
MESH = pl.DeviceIdType.MESH

BLOCK = 32
CHILDREN = {
    0: (9, 3, 5, 1),
    3: (19, 6, 2),
    5: (7, 13, 4),
    7: (14,),
    9: (21, 17, 11),
    11: (15, 10),
    13: (8, 12),
    17: (25, 16),
    19: (23, 27, 18),
    21: (31, 29, 20),
    23: (22,),
    25: (24,),
    27: (26,),
    29: (28,),
    31: (30,),
}
RELAYS = {3: 1, 5: 2, 7: 3, 9: 2, 11: 3, 13: 3, 17: 3, 19: 3, 21: 3, 23: 4, 25: 4, 27: 3, 29: 4, 31: 4}


def plan(n):
    if n % BLOCK == 0:
        return BLOCK, CHILDREN, RELAYS
    chain = {d: (d + 1,) for d in range(n - 1)}
    return n, chain, {d: 4 for d in range(1, n - 1)}


def pick(here, table):
    value = 0
    for place, entry in table.items():
        value = jnp.where(here == place, entry, value)
    return value


def packed(fields, base):
    return sum(field * base**i for i, field in enumerate(fields))


def kernel(
    n,
    q_hbm,
    k_hbm,
    v_hbm,
    out,
    q,
    loc,
    halo,
    anc,
    acc,
    total,
    top,
    q_sem,
    loc_sem,
    halo_sem,
    send_sem,
    recv_sem,
):
    me = lax.axis_index("seq")
    tokens = q_hbm.shape[0]
    heads = q_hbm.shape[1] // HEAD_SIZE
    group = heads // KEY_VALUE_HEADS
    factor = math.log2(math.e) / math.sqrt(HEAD_SIZE)
    every = tuple(range(KEY_VALUE_HEADS))

    for h in every:
        columns = pl.ds(h * HEAD_SIZE, HEAD_SIZE)
        for side, ref in enumerate((k_hbm, v_hbm)):
            pltpu.make_async_copy(ref.at[:, columns], loc.at[h, side], loc_sem).start()
    query_copy = pltpu.make_async_copy(q_hbm, q, q_sem)
    query_copy.start()

    block, tree, relays = plan(n)
    here = me % block
    origin = me - here
    base = block + 1
    above = {d: set() for d in range(block)}
    for d, below in tree.items():
        for child in below:
            above[child].add(d)
    for d in range(1, block):
        above[d].add(d - 1)
    ready_table = {
        d: sum(d in others for others in above.values()) for d in range(block)
    }

    barrier = pltpu.get_barrier_semaphore()
    most = max(len(others) for others in above.values())
    parents = pick(
        here, {d: packed([p + 1 for p in sorted(o)], base) for d, o in above.items()}
    )
    for i in range(most):
        parent = (parents // base**i) % base

        @pl.when(parent > 0)
        def _(parent=parent):
            pl.semaphore_signal(
                barrier,
                inc=1,
                device_id=(origin + parent - 1,),
                device_id_type=MESH,
            )

    ready = pick(here, ready_table)
    if n > block:
        @pl.when((here == 0) & (me > 0))
        def _():
            for target in (me - block, me - 1):
                pl.semaphore_signal(
                    barrier, inc=1, device_id=(target,), device_id_type=MESH
                )

        across = jnp.where((here == 0) | (here == block - 1), 1, 0)
        ready = ready + jnp.where(me + block < n, across, 0)
        ready = ready + jnp.where(
            (here == block - 1) & (me + block >= n) & (me < n - 1), 1, 0
        )

    slots = max(len(below) for below in tree.values())
    code = pick(
        here, {d: packed([c + 1 for c in below], base) for d, below in tree.items()}
    )
    children = []
    for i in range(slots):
        child = (code // base**i) % base
        children.append((child > 0, origin + child - 1))
    turn = pick(here, relays)
    if n > block:
        turn = jnp.where((here == 0) & (me > 0), 1, turn)
        children.append(((here == 0) & (me + block < n), me + block))

    def to_child(source, target, slot, arrival):
        return pltpu.make_async_remote_copy(
            src_ref=source,
            dst_ref=target,
            send_sem=send_sem.at[slot],
            recv_sem=arrival,
            device_id=(children[slot][1],),
            device_id_type=MESH,
        )

    def forward(source, h, side):
        for slot, (condition, _) in enumerate(children):

            @pl.when(condition)
            def _(slot=slot):
                to_child(
                    source.at[h, side], anc.at[h, side], slot, recv_sem.at[h, side]
                ).start()

    @pl.when(ready > 0)
    def _():
        pl.semaphore_wait(barrier, ready)

    pltpu.make_async_copy(loc, loc, loc_sem).wait()

    halo_copy = pltpu.make_async_remote_copy(
        src_ref=loc.at[:, :, pl.ds(tokens - HALO, HALO)],
        dst_ref=halo,
        send_sem=halo_sem.at[0],
        recv_sem=halo_sem.at[1],
        device_id=((me + 1) % n,),
        device_id_type=MESH,
    )

    @pl.when(me == 0)
    def _():
        for h in every:
            for side in range(2):
                forward(loc, h, side)

    @pl.when(me < n - 1)
    def _():
        halo_copy.start()

    def take(h, side):
        pltpu.make_async_remote_copy(
            src_ref=anc.at[h, side],
            dst_ref=anc.at[h, side],
            send_sem=send_sem.at[0],
            recv_sem=recv_sem.at[h, side],
            device_id=((me + 1) % n,),
            device_id_type=MESH,
        ).wait_recv()

    def pass_on(h):
        for side in range(2):
            take(h, side)
            forward(anc, h, side)

    def relay(which):
        @pl.when(turn == which)
        def _():
            for h in every:
                pass_on(h)

    rows = group * tokens

    def stacked(h):
        first = h * group
        return jnp.concatenate(
            [
                q[:, (first + i) * HEAD_SIZE : (first + i + 1) * HEAD_SIZE]
                for i in range(group)
            ],
            axis=0,
        )

    def scores(h, key):
        return lax.dot_general(
            key, stacked(h), (((1,), (1,)), ((), ())), preferred_element_type=jnp.float32
        )

    def flipped(value):
        ones = jnp.ones((2 * SUM_ROWS, value.shape[0]), value.dtype)
        return jnp.concatenate([value.T, ones], axis=0)

    def mix(weights, value):
        both = jnp.dot(
            flipped(value),
            weights.astype(jnp.bfloat16),
            preferred_element_type=jnp.float32,
        )
        return both[:HEAD_SIZE], both[HEAD_SIZE : HEAD_SIZE + SUM_ROWS]

    def put(h, mixed, summed):
        first = h * group
        result = (mixed * (1.0 / summed[:1])).astype(out.dtype)
        for i in range(group):
            out[:, (first + i) * HEAD_SIZE : (first + i + 1) * HEAD_SIZE] = result[
                :, i * tokens : (i + 1) * tokens
            ].T

    relay(1)

    key_ids = lax.broadcasted_iota(jnp.int32, (tokens, rows), 0)
    query_ids = lax.broadcasted_iota(jnp.int32, (tokens, rows), 1) % tokens
    visible = key_ids <= query_ids
    query_copy.wait()
    for h in every:
        s = jnp.where(visible, scores(h, loc[h, 0]), -1e30)
        highest = jnp.max(s, axis=0, keepdims=True)
        mixed, summed = mix(jnp.exp2((s - highest) * factor), loc[h, 1])
        acc[h] = mixed
        total[h] = summed
        top[h] = jnp.broadcast_to(highest, (SUM_ROWS, rows))

    @pl.when(me == 0)
    def _():
        for h in every:
            put(h, acc[h], total[h])

    relay(2)

    def merged(h, key, value):
        s = scores(h, key)
        before = top[h]
        highest = jnp.maximum(before, jnp.max(s, axis=0, keepdims=True))
        drop = jnp.exp2((before - highest) * factor)
        mixed, summed = mix(jnp.exp2((s - highest[:1]) * factor), value)
        mixed = mixed + acc[h] * drop[:1]
        summed = summed + total[h] * drop
        return mixed, summed, highest

    @pl.when(me > 0)
    def _():
        halo_copy.wait_recv()
        for h in every:
            mixed, summed, highest = merged(h, halo[h, 0], halo[h, 1])
            acc[h] = mixed
            total[h] = summed
            top[h] = highest
        relay(3)
        for h in every:

            @pl.when(turn == 0)
            def _(h=h):
                for side in range(2):
                    take(h, side)

            @pl.when(turn == 4)
            def _(h=h):
                pass_on(h)

            mixed, summed, _ = merged(h, anc[h, 0], anc[h, 1])
            put(h, mixed, summed)

    @pl.when((turn > 0) | (me == 0))
    def _():
        for slot, (condition, _) in enumerate(children):

            @pl.when(condition)
            def _(slot=slot):
                to_child(anc, anc, slot, recv_sem.at[0, 0]).wait_send()

    @pl.when(me < n - 1)
    def _():
        halo_copy.wait_send()


def attention(n, queries, keys, values):
    tokens, width = queries.shape
    rows = width // HEAD_SIZE // KEY_VALUE_HEADS * tokens
    block, tree, _ = plan(n)
    slots = max(len(below) for below in tree.values()) + (n > block)
    state = pltpu.VMEM((KEY_VALUE_HEADS, HEAD_SIZE, rows), jnp.float32)
    row = pltpu.VMEM((KEY_VALUE_HEADS, SUM_ROWS, rows), jnp.float32)
    pieces = (KEY_VALUE_HEADS, 2, tokens, HEAD_SIZE)
    return pl.pallas_call(
        functools.partial(kernel, n),
        out_shape=pltpu.VMEM(queries.shape, queries.dtype),
        in_specs=[pl.BlockSpec(memory_space=pltpu.HBM)] * 3,
        out_specs=pl.BlockSpec(memory_space=pltpu.VMEM),
        scratch_shapes=[
            pltpu.VMEM(queries.shape, queries.dtype),
            pltpu.VMEM(pieces, keys.dtype),
            pltpu.VMEM((KEY_VALUE_HEADS, 2, HALO, HEAD_SIZE), keys.dtype),
            pltpu.VMEM(pieces, keys.dtype),
            state,
            row,
            row,
            pltpu.SemaphoreType.DMA,
            pltpu.SemaphoreType.DMA,
            pltpu.SemaphoreType.DMA((2,)),
            pltpu.SemaphoreType.DMA((slots,)),
            pltpu.SemaphoreType.DMA((KEY_VALUE_HEADS, 2)),
        ],
        compiler_params=pltpu.CompilerParams(
            collective_id=0, has_side_effects=True, vmem_limit_bytes=60 * 2**20
        ),
    )(queries, keys, values)


def solution(mesh):
    n = mesh.shape["seq"]
    return jax.shard_map(
        functools.partial(attention, n),
        mesh=mesh,
        in_specs=(P("seq", None), P("seq", None), P("seq", None)),
        out_specs=P("seq", None),
        check_vma=False,
    )
```

```python
import functools
import math

import jax
import jax.numpy as jnp
from jax import lax
from jax.experimental import pallas as pl
from jax.experimental.pallas import tpu as pltpu
from jax.sharding import PartitionSpec as P

KEY_VALUE_HEADS = 4
HEAD_SIZE = 128
HALO = 64
SUM_ROWS = 8
MESH = pl.DeviceIdType.MESH

BLOCK = 32
KEY_CHILDREN = {
    0: (3, 5, 9, 1,),
    1: (15,),
    3: (27, 7, 2,),
    5: (13, 4,),
    7: (23, 6,),
    9: (17, 11, 8,),
    11: (10,),
    13: (29, 12,),
    15: (14,),
    17: (19, 21, 25, 16,),
    19: (18,),
    21: (20,),
    23: (22,),
    25: (24,),
    27: (31, 26,),
    29: (28,),
    31: (30,),
}
VALUE_CHILDREN = {
    0: (3, 9, 5, 1,),
    3: (27, 7, 2,),
    5: (4,),
    7: (23, 6,),
    9: (13, 17, 11, 8,),
    11: (10,),
    13: (29, 15, 12,),
    15: (14,),
    17: (19, 21, 25, 16,),
    19: (18,),
    21: (20,),
    23: (22,),
    25: (24,),
    27: (31, 26,),
    29: (28,),
    31: (30,),
}
TURN = {1: 2, 3: 1, 5: 2, 7: 3, 9: 1, 11: 4, 13: 3, 15: 4, 17: 3, 19: 4, 21: 4, 23: 4, 25: 4, 27: 2, 29: 4, 31: 4}
LATE_HALO = {1: 1, 2: 1, 4: 1, 21: 1, 27: 1}
HALO_LAST = (2, 4, 8, 26, )


def plan(n):
    if n % BLOCK == 0:
        return BLOCK, (KEY_CHILDREN, VALUE_CHILDREN), TURN, LATE_HALO, HALO_LAST
    chain = {d: (d + 1,) for d in range(n - 1)}
    return n, (chain, chain), {d: 4 for d in range(1, n - 1)}, {}, ()


def pick(here, table):
    value = 0
    for place, entry in table.items():
        value = jnp.where(here == place, entry, value)
    return value


def packed(fields, base):
    return sum(field * base**i for i, field in enumerate(fields))


def kernel(
    n,
    q_hbm,
    k_hbm,
    v_hbm,
    out,
    q,
    loc,
    halo,
    anc,
    acc,
    total,
    top,
    q_sem,
    loc_sem,
    halo_sem,
    send_sem,
    recv_sem,
):
    me = lax.axis_index("seq")
    tokens = q_hbm.shape[0]
    heads = q_hbm.shape[1] // HEAD_SIZE
    group = heads // KEY_VALUE_HEADS
    factor = math.log2(math.e) / math.sqrt(HEAD_SIZE)
    every = tuple(range(KEY_VALUE_HEADS))

    for h in every:
        columns = pl.ds(h * HEAD_SIZE, HEAD_SIZE)
        for side, ref in enumerate((k_hbm, v_hbm)):
            pltpu.make_async_copy(ref.at[:, columns], loc.at[h, side], loc_sem).start()
    query_copy = pltpu.make_async_copy(q_hbm, q, q_sem)
    query_copy.start()

    block, trees, turns, late_halo, halo_last = plan(n)
    here = me % block
    origin = me - here
    base = block + 1
    above = {d: set() for d in range(block)}
    for tree in trees:
        for d, below in tree.items():
            for child in below:
                above[child].add(d)
    for d in range(1, block):
        above[d].add(d - 1)
    ready_table = {
        d: sum(d in others for others in above.values()) for d in range(block)
    }

    barrier = pltpu.get_barrier_semaphore()
    most = max(len(others) for others in above.values())
    parents = pick(
        here, {d: packed([p + 1 for p in sorted(o)], base) for d, o in above.items()}
    )
    for i in range(most):
        parent = (parents // base**i) % base

        @pl.when(parent > 0)
        def _(parent=parent):
            pl.semaphore_signal(
                barrier,
                inc=1,
                device_id=(origin + parent - 1,),
                device_id_type=MESH,
            )

    ready = pick(here, ready_table)
    if n > block:
        @pl.when((here == 0) & (me > 0))
        def _():
            for target in (me - block, me - 1):
                pl.semaphore_signal(
                    barrier, inc=1, device_id=(target,), device_id_type=MESH
                )

        across = jnp.where((here == 0) | (here == block - 1), 1, 0)
        ready = ready + jnp.where(me + block < n, across, 0)
        ready = ready + jnp.where(
            (here == block - 1) & (me + block >= n) & (me < n - 1), 1, 0
        )

    slots = max(len(below) for tree in trees for below in tree.values())
    children = []
    for tree in trees:
        code = pick(
            here, {d: packed([c + 1 for c in below], base) for d, below in tree.items()}
        )
        targets = []
        for i in range(slots):
            child = (code // base**i) % base
            targets.append((child > 0, origin + child - 1))
        if n > block:
            targets.append(((here == 0) & (me + block < n), me + block))
        children.append(targets)
    turn = pick(here, turns)
    late = pick(here, late_halo)
    last = pick(here, {d: 1 for d in halo_last})
    if n > block:
        turn = jnp.where((here == 0) & (me > 0), 1, turn)

    def to_child(source, target, slot, side, arrival):
        return pltpu.make_async_remote_copy(
            src_ref=source,
            dst_ref=target,
            send_sem=send_sem.at[slot, side],
            recv_sem=arrival,
            device_id=(children[side][slot][1],),
            device_id_type=MESH,
        )

    def forward(source, h, side):
        for slot, (condition, _) in enumerate(children[side]):

            @pl.when(condition)
            def _(slot=slot):
                to_child(
                    source.at[h, side], anc.at[h, side], slot, side, recv_sem.at[h, side]
                ).start()

    @pl.when(ready > 0)
    def _():
        pl.semaphore_wait(barrier, ready)

    pltpu.make_async_copy(loc, loc, loc_sem).wait()

    halo_copy = pltpu.make_async_remote_copy(
        src_ref=loc.at[:, :, pl.ds(tokens - HALO, HALO)],
        dst_ref=halo,
        send_sem=halo_sem.at[0],
        recv_sem=halo_sem.at[1],
        device_id=((me + 1) % n,),
        device_id_type=MESH,
    )

    @pl.when(me == 0)
    def _():
        for h in every:
            for side in range(2):
                forward(loc, h, side)

    def send_halo(which):
        @pl.when((me < n - 1) & (late == which))
        def _():
            halo_copy.start()

    send_halo(0)

    def take(h, side):
        pltpu.make_async_remote_copy(
            src_ref=anc.at[h, side],
            dst_ref=anc.at[h, side],
            send_sem=send_sem.at[0],
            recv_sem=recv_sem.at[h, side],
            device_id=((me + 1) % n,),
            device_id_type=MESH,
        ).wait_recv()

    def pass_on(h):
        for side in range(2):
            take(h, side)
            forward(anc, h, side)

    def relay(which):
        @pl.when(turn == which)
        def _():
            for h in every:
                pass_on(h)

    rows = group * tokens

    def stacked(h):
        first = h * group
        return jnp.concatenate(
            [
                q[:, (first + i) * HEAD_SIZE : (first + i + 1) * HEAD_SIZE]
                for i in range(group)
            ],
            axis=0,
        )

    def scores(h, key):
        return lax.dot_general(
            key, stacked(h), (((1,), (1,)), ((), ())), preferred_element_type=jnp.float32
        )

    def flipped(value):
        ones = jnp.ones((2 * SUM_ROWS, value.shape[0]), value.dtype)
        return jnp.concatenate([value.T, ones], axis=0)

    def mix(weights, value):
        both = jnp.dot(
            flipped(value),
            weights.astype(jnp.bfloat16),
            preferred_element_type=jnp.float32,
        )
        return both[:HEAD_SIZE], both[HEAD_SIZE : HEAD_SIZE + SUM_ROWS]

    def put(h, mixed, summed):
        first = h * group
        result = (mixed * (1.0 / summed[:1])).astype(out.dtype)
        for i in range(group):
            out[:, (first + i) * HEAD_SIZE : (first + i + 1) * HEAD_SIZE] = result[
                :, i * tokens : (i + 1) * tokens
            ].T

    relay(1)
    send_halo(3)

    key_ids = lax.broadcasted_iota(jnp.int32, (tokens, rows), 0)
    query_ids = lax.broadcasted_iota(jnp.int32, (tokens, rows), 1) % tokens
    visible = key_ids <= query_ids
    query_copy.wait()
    for h in every:
        s = jnp.where(visible, scores(h, loc[h, 0]), -1e30)
        highest = jnp.max(s, axis=0, keepdims=True)
        mixed, summed = mix(jnp.exp2((s - highest) * factor), loc[h, 1])
        acc[h] = mixed
        total[h] = summed
        top[h] = jnp.broadcast_to(highest, (SUM_ROWS, rows))

    @pl.when(me == 0)
    def _():
        for h in every:
            put(h, acc[h], total[h])

    send_halo(1)
    relay(2)
    send_halo(2)

    def merged(h, key, value):
        s = scores(h, key)
        before = top[h]
        highest = jnp.maximum(before, jnp.max(s, axis=0, keepdims=True))
        drop = jnp.exp2((before - highest) * factor)
        mixed, summed = mix(jnp.exp2((s - highest[:1]) * factor), value)
        mixed = mixed + acc[h] * drop[:1]
        summed = summed + total[h] * drop
        return mixed, summed, highest

    def keep(h, mixed, summed, highest):
        acc[h] = mixed
        total[h] = summed
        top[h] = highest

    def take_head(h):
        @pl.when(turn == 0)
        def _():
            for side in range(2):
                take(h, side)

        @pl.when(turn == 4)
        def _():
            pass_on(h)

    @pl.when((me > 0) & (last == 0))
    def _():
        halo_copy.wait_recv()
        for h in every:
            keep(h, *merged(h, halo[h, 0], halo[h, 1]))
        relay(3)
        for h in every:
            take_head(h)
            mixed, summed, _ = merged(h, anc[h, 0], anc[h, 1])
            put(h, mixed, summed)

    if halo_last:

        @pl.when((me > 0) & (last == 1))
        def _():
            for h in every:
                take_head(h)
                keep(h, *merged(h, anc[h, 0], anc[h, 1]))
            halo_copy.wait_recv()
            for h in every:
                mixed, summed, _ = merged(h, halo[h, 0], halo[h, 1])
                put(h, mixed, summed)

    @pl.when((turn > 0) | (me == 0))
    def _():
        for side in range(2):
            for slot, (condition, _) in enumerate(children[side]):

                @pl.when(condition)
                def _(slot=slot, side=side):
                    half = anc.at[:, side]
                    to_child(half, half, slot, side, recv_sem.at[0, 0]).wait_send()

    @pl.when(me < n - 1)
    def _():
        halo_copy.wait_send()


def attention(n, queries, keys, values):
    tokens, width = queries.shape
    rows = width // HEAD_SIZE // KEY_VALUE_HEADS * tokens
    block, trees, *_ = plan(n)
    slots = max(len(below) for tree in trees for below in tree.values()) + (n > block)
    state = pltpu.VMEM((KEY_VALUE_HEADS, HEAD_SIZE, rows), jnp.float32)
    row = pltpu.VMEM((KEY_VALUE_HEADS, SUM_ROWS, rows), jnp.float32)
    pieces = (KEY_VALUE_HEADS, 2, tokens, HEAD_SIZE)
    return pl.pallas_call(
        functools.partial(kernel, n),
        out_shape=pltpu.VMEM(queries.shape, queries.dtype),
        in_specs=[pl.BlockSpec(memory_space=pltpu.HBM)] * 3,
        out_specs=pl.BlockSpec(memory_space=pltpu.VMEM),
        scratch_shapes=[
            pltpu.VMEM(queries.shape, queries.dtype),
            pltpu.VMEM(pieces, keys.dtype),
            pltpu.VMEM((KEY_VALUE_HEADS, 2, HALO, HEAD_SIZE), keys.dtype),
            pltpu.VMEM(pieces, keys.dtype),
            state,
            row,
            row,
            pltpu.SemaphoreType.DMA,
            pltpu.SemaphoreType.DMA,
            pltpu.SemaphoreType.DMA((2,)),
            pltpu.SemaphoreType.DMA((slots, 2)),
            pltpu.SemaphoreType.DMA((KEY_VALUE_HEADS, 2)),
        ],
        compiler_params=pltpu.CompilerParams(
            collective_id=0, has_side_effects=True, vmem_limit_bytes=60 * 2**20
        ),
    )(queries, keys, values)


def solution(mesh):
    n = mesh.shape["seq"]
    return jax.shard_map(
        functools.partial(attention, n),
        mesh=mesh,
        in_specs=(P("seq", None), P("seq", None), P("seq", None)),
        out_specs=P("seq", None),
        check_vma=False,
    )
```

```python
import functools
import math

import jax
import jax.numpy as jnp
from jax import lax
from jax.experimental import pallas as pl
from jax.experimental.pallas import tpu as pltpu
from jax.sharding import PartitionSpec as P

KEY_VALUE_HEADS = 4
HEAD_SIZE = 128
HALO = 64
SUM_ROWS = 8
MESH = pl.DeviceIdType.MESH

BLOCK = 32
KEY_CHILDREN = {
    0: (9, 5, 3, 1,),
    3: (27, 7, 2,),
    5: (29, 4,),
    7: (23, 6,),
    9: (13, 8, 11, 17,),
    11: (10,),
    13: (12, 15,),
    15: (14,),
    17: (21, 19, 25, 16,),
    19: (18,),
    21: (20,),
    23: (22,),
    25: (24,),
    27: (26, 31,),
    29: (28,),
    31: (30,),
}
VALUE_CHILDREN = {
    0: (5, 3, 9, 1,),
    1: (14,),
    3: (27, 7, 2,),
    5: (29, 4,),
    7: (23, 6,),
    9: (11, 13, 17, 8,),
    11: (10,),
    13: (15, 12,),
    17: (21, 19, 25, 16,),
    19: (18,),
    21: (20,),
    23: (22,),
    25: (24,),
    27: (26, 31,),
    29: (28,),
    31: (30,),
}
TURN = {0: 5, 1: 4, 2: 1, 3: 0, 4: 4, 5: 1, 6: 3, 7: 4, 8: 4, 9: 0, 10: 3, 11: 4, 12: 3, 13: 2, 14: 3, 15: 3, 16: 4, 17: 0, 18: 4, 19: 4, 20: 3, 21: 3, 22: 4, 23: 4, 24: 4, 25: 4, 26: 4, 27: 1, 28: 4, 29: 4, 30: 3, 31: 3}
LATE_HALO = {1: 1, 4: 1, 8: 1, 15: 1, 16: 1, 20: 1, 24: 1, 25: 1, 26: 1, 27: 1, 29: 1}


def plan(n):
    if n % BLOCK == 0:
        return BLOCK, (KEY_CHILDREN, VALUE_CHILDREN), TURN, LATE_HALO
    chain = {d: (d + 1,) for d in range(n - 1)}
    return n, (chain, chain), {d: 3 if d else 5 for d in range(n)}, {}


def pick(here, table):
    value = 0
    for place, entry in table.items():
        value = jnp.where(here == place, entry, value)
    return value


def packed(fields, base):
    return sum(field * base**i for i, field in enumerate(fields))


def kernel(
    n,
    q_hbm,
    k_hbm,
    v_hbm,
    out,
    q,
    flat,
    kv,
    acc,
    total,
    top,
    q_sem,
    loc_sem,
    halo_sem,
    send_sem,
    recv_sem,
):
    me = lax.axis_index("seq")
    tokens = q_hbm.shape[0]
    heads = q_hbm.shape[1] // HEAD_SIZE
    group = heads // KEY_VALUE_HEADS
    factor = math.log2(math.e) / math.sqrt(HEAD_SIZE)
    every = tuple(range(KEY_VALUE_HEADS))
    rows = group * tokens

    before = tokens + HALO
    anchor = pl.ds(0, tokens)
    halo = pl.ds(tokens, HALO)
    own = pl.ds(before, tokens)

    for h in every:
        columns = pl.ds(h * HEAD_SIZE, HEAD_SIZE)
        for side, ref in enumerate((k_hbm, v_hbm)):
            pltpu.make_async_copy(
                ref.at[:, columns], kv.at[h, side, own], loc_sem
            ).start()
    query_copy = pltpu.make_async_copy(q_hbm, q, q_sem)
    query_copy.start()

    block, trees, turns, late_halo = plan(n)
    here = me % block
    origin = me - here
    base = block + 1
    above = {d: set() for d in range(block)}
    for tree in trees:
        for d, below in tree.items():
            for child in below:
                above[child].add(d)
    for d in range(1, block):
        above[d].add(d - 1)
    ready_table = {
        d: sum(d in others for others in above.values()) for d in range(block)
    }

    barrier = pltpu.get_barrier_semaphore()
    most = max(len(others) for others in above.values())
    parents = pick(
        here, {d: packed([p + 1 for p in sorted(o)], base) for d, o in above.items()}
    )
    for i in range(most):
        parent = (parents // base**i) % base

        @pl.when(parent > 0)
        def _(parent=parent):
            pl.semaphore_signal(
                barrier,
                inc=1,
                device_id=(origin + parent - 1,),
                device_id_type=MESH,
            )

    ready = pick(here, ready_table)
    if n > block:
        @pl.when((here == 0) & (me > 0))
        def _():
            for target in (me - block, me - 1):
                pl.semaphore_signal(
                    barrier, inc=1, device_id=(target,), device_id_type=MESH
                )

        across = jnp.where((here == 0) | (here == block - 1), 1, 0)
        ready = ready + jnp.where(me + block < n, across, 0)
        ready = ready + jnp.where(
            (here == block - 1) & (me + block >= n) & (me < n - 1), 1, 0
        )

    slots = max(len(below) for tree in trees for below in tree.values())
    children = []
    for tree in trees:
        code = pick(
            here, {d: packed([c + 1 for c in below], base) for d, below in tree.items()}
        )
        targets = []
        for i in range(slots):
            child = (code // base**i) % base
            targets.append((child > 0, origin + child - 1))
        if n > block:
            targets.append(((here == 0) & (me + block < n), me + block))
        children.append(targets)
    turn = pick(here, turns)
    late = pick(here, late_halo)
    if n > block:
        turn = jnp.where((here == 0) & (me > 0), 0, turn)

    def to_child(rows_sent, h, slot, side):
        return pltpu.make_async_remote_copy(
            src_ref=kv.at[h, side, rows_sent],
            dst_ref=kv.at[h, side, anchor],
            send_sem=send_sem.at[slot, side],
            recv_sem=recv_sem.at[h, side],
            device_id=(children[side][slot][1],),
            device_id_type=MESH,
        )

    def forward(rows_sent, h, side):
        for slot, (condition, _) in enumerate(children[side]):

            @pl.when(condition)
            def _(slot=slot):
                to_child(rows_sent, h, slot, side).start()

    query_copy.wait()
    for i in range(heads):
        flat[:, i * tokens : (i + 1) * tokens] = q[
            :, i * HEAD_SIZE : (i + 1) * HEAD_SIZE
        ].T

    @pl.when(ready > 0)
    def _():
        pl.semaphore_wait(barrier, ready)

    pltpu.make_async_copy(kv.at[:, :, own], kv.at[:, :, own], loc_sem).wait()

    halo_copy = pltpu.make_async_remote_copy(
        src_ref=kv.at[:, :, pl.ds(before + tokens - HALO, HALO)],
        dst_ref=kv.at[:, :, halo],
        send_sem=halo_sem.at[0],
        recv_sem=halo_sem.at[1],
        device_id=((me + 1) % n,),
        device_id_type=MESH,
    )

    def send_halo(which):
        @pl.when((me < n - 1) & (late == which))
        def _():
            halo_copy.start()

    send_halo(0)

    @pl.when(me == 0)
    def _():
        for h in every:
            for side in range(2):
                forward(own, h, side)

    def pass_on(h):
        for side in range(2):
            pltpu.make_async_remote_copy(
                src_ref=kv.at[h, side, anchor],
                dst_ref=kv.at[h, side, anchor],
                send_sem=send_sem.at[0, side],
                recv_sem=recv_sem.at[h, side],
                device_id=((me + 1) % n,),
                device_id_type=MESH,
            ).wait_recv()
            forward(anchor, h, side)

    def pass_all():
        for h in every:
            pass_on(h)

    def scores(h, first, stop):
        return jnp.dot(
            kv[h, 0, first:stop],
            flat[:, h * rows : (h + 1) * rows],
            preferred_element_type=jnp.float32,
        )

    def weigh(s, highest):
        return jnp.exp2((s - highest) * factor).astype(jnp.bfloat16)

    def mix(h, first, stop, weights):
        value = kv[h, 1, first:stop]
        ones = jnp.ones((2 * SUM_ROWS, stop - first), value.dtype)
        both = jnp.dot(
            jnp.concatenate([value.T, ones], axis=0),
            weights,
            preferred_element_type=jnp.float32,
        )
        return both[:HEAD_SIZE], both[HEAD_SIZE : HEAD_SIZE + SUM_ROWS]

    def put(h, mixed, summed):
        first = h * group
        result = (mixed * (1.0 / summed[:1])).astype(out.dtype)
        for i in range(group):
            out[:, (first + i) * HEAD_SIZE : (first + i + 1) * HEAD_SIZE] = result[
                :, i * tokens : (i + 1) * tokens
            ].T

    def keep(h, mixed, summed, highest):
        acc[h] = mixed
        total[h] = summed
        top[h] = jnp.broadcast_to(highest, (SUM_ROWS, rows))

    def merged(h, first, stop):
        s = scores(h, first, stop)
        was = top[h]
        highest = jnp.maximum(was, jnp.max(s, axis=0, keepdims=True))
        drop = jnp.exp2((was - highest) * factor)
        mixed, summed = mix(h, first, stop, weigh(s, highest[:1]))
        mixed = mixed + acc[h] * drop[:1]
        summed = summed + total[h] * drop
        return mixed, summed, highest

    key_ids = lax.broadcasted_iota(jnp.int32, (tokens, rows), 0)
    query_ids = lax.broadcasted_iota(jnp.int32, (tokens, rows), 1) % tokens
    visible = key_ids <= query_ids

    @pl.when(turn == 0)
    def _():
        pass_all()
        send_halo(3)
        halo_copy.wait_recv()
        for h in every:
            s = scores(h, 0, before + tokens)
            others, mine = s[:before], jnp.where(visible, s[before:], -1e30)
            highest = jnp.maximum(
                jnp.max(others, axis=0, keepdims=True),
                jnp.max(mine, axis=0, keepdims=True),
            )
            weights = jnp.concatenate(
                [weigh(others, highest), weigh(mine, highest)], axis=0
            )
            put(h, *mix(h, 0, before + tokens, weights))

    @pl.when(turn > 0)
    def _():
        for h in every:
            s = jnp.where(visible, scores(h, before, before + tokens), -1e30)
            highest = jnp.max(s, axis=0, keepdims=True)
            mixed, summed = mix(h, before, before + tokens, weigh(s, highest))
            keep(h, mixed, summed, highest)

    @pl.when(me == 0)
    def _():
        for h in every:
            put(h, acc[h], total[h])

    send_halo(1)

    @pl.when(turn == 1)
    def _():
        pass_all()
        send_halo(2)

    @pl.when((turn == 1) | (turn == 4))
    def _():
        halo_copy.wait_recv()
        for h in every:

            @pl.when(turn == 4)
            def _(h=h):
                pass_on(h)

            mixed, summed, _ = merged(h, 0, before)
            put(h, mixed, summed)

    @pl.when((turn == 2) | (turn == 3))
    def _():
        halo_copy.wait_recv()
        for h in every:
            keep(h, *merged(h, tokens, before))

        @pl.when(turn == 2)
        def _():
            pass_all()

        for h in every:

            @pl.when(turn == 3)
            def _(h=h):
                pass_on(h)

            mixed, summed, _ = merged(h, 0, tokens)
            put(h, mixed, summed)

    for side in range(2):
        for slot, (condition, _) in enumerate(children[side]):

            @pl.when(condition)
            def _(slot=slot, side=side):
                sent = kv.at[:, side, anchor]
                pltpu.make_async_remote_copy(
                    src_ref=sent,
                    dst_ref=sent,
                    send_sem=send_sem.at[slot, side],
                    recv_sem=recv_sem.at[0, side],
                    device_id=(children[side][slot][1],),
                    device_id_type=MESH,
                ).wait_send()

    @pl.when(me < n - 1)
    def _():
        halo_copy.wait_send()


def attention(n, queries, keys, values):
    tokens, width = queries.shape
    rows = width // HEAD_SIZE // KEY_VALUE_HEADS * tokens
    block, trees, *_ = plan(n)
    slots = max(len(below) for tree in trees for below in tree.values()) + (n > block)
    state = pltpu.VMEM((KEY_VALUE_HEADS, HEAD_SIZE, rows), jnp.float32)
    row = pltpu.VMEM((KEY_VALUE_HEADS, SUM_ROWS, rows), jnp.float32)
    pieces = (KEY_VALUE_HEADS, 2, 2 * tokens + HALO, HEAD_SIZE)
    return pl.pallas_call(
        functools.partial(kernel, n),
        out_shape=pltpu.VMEM(queries.shape, queries.dtype),
        in_specs=[pl.BlockSpec(memory_space=pltpu.HBM)] * 3,
        out_specs=pl.BlockSpec(memory_space=pltpu.VMEM),
        scratch_shapes=[
            pltpu.VMEM(queries.shape, queries.dtype),
            pltpu.VMEM((HEAD_SIZE, KEY_VALUE_HEADS * rows), queries.dtype),
            pltpu.VMEM(pieces, keys.dtype),
            state,
            row,
            row,
            pltpu.SemaphoreType.DMA,
            pltpu.SemaphoreType.DMA,
            pltpu.SemaphoreType.DMA((2,)),
            pltpu.SemaphoreType.DMA((slots, 2)),
            pltpu.SemaphoreType.DMA((KEY_VALUE_HEADS, 2)),
        ],
        compiler_params=pltpu.CompilerParams(
            collective_id=0, has_side_effects=True, vmem_limit_bytes=60 * 2**20
        ),
    )(queries, keys, values)


def solution(mesh):
    n = mesh.shape["seq"]
    return jax.shard_map(
        functools.partial(attention, n),
        mesh=mesh,
        in_specs=(P("seq", None), P("seq", None), P("seq", None)),
        out_specs=P("seq", None),
        check_vma=False,
    )
```

```python
import functools
import math

import jax
import jax.numpy as jnp
from jax import lax
from jax.experimental import pallas as pl
from jax.experimental.pallas import tpu as pltpu
from jax.sharding import PartitionSpec as P

KEY_VALUE_HEADS = 4
HEAD_SIZE = 128
HALO = 64
SUM_ROWS = 8
PARTS = 2
MESH = pl.DeviceIdType.MESH

BLOCK = 32
KEY_CHILDREN = {
    0: (9, 5, 3, 1,),
    3: (27, 7, 2,),
    5: (29, 4,),
    7: (23, 6,),
    9: (11, 8, 13, 17,),
    11: (10, 15,),
    13: (12,),
    15: (14,),
    17: (21, 19, 25, 16,),
    19: (18,),
    21: (20,),
    23: (22,),
    25: (24,),
    27: (26, 31,),
    29: (28,),
    31: (30,),
}
VALUE_CHILDREN = {
    0: (5, 3, 9, 1,),
    3: (27, 7, 2,),
    5: (29, 4,),
    7: (23, 6,),
    9: (11, 17, 13, 8,),
    11: (15, 10,),
    13: (12,),
    15: (14,),
    17: (21, 19, 25, 16,),
    19: (18,),
    21: (20,),
    23: (22,),
    25: (24,),
    27: (26, 31,),
    29: (28,),
    31: (30,),
}
TURN = {0: 5, 1: 3, 2: 1, 3: 0, 4: 4, 5: 1, 6: 3, 7: 4, 8: 4, 9: 0, 10: 3, 11: 2, 12: 3, 13: 3, 14: 3, 15: 3, 16: 4, 17: 0, 18: 4, 19: 4, 20: 3, 21: 3, 22: 4, 23: 4, 24: 4, 25: 4, 26: 4, 27: 1, 28: 4, 29: 4, 30: 3, 31: 3}
LATE_HALO = {1: 4, 4: 1, 8: 1, 15: 1, 16: 1, 20: 1, 24: 1, 25: 1, 26: 1, 27: 1, 29: 1}


def plan(n):
    if n % BLOCK == 0:
        return BLOCK, (KEY_CHILDREN, VALUE_CHILDREN), TURN, LATE_HALO
    chain = {d: (d + 1,) for d in range(n - 1)}
    return n, (chain, chain), {d: 3 if d else 5 for d in range(n)}, {}


def pick(here, table):
    value = 0
    for place, entry in table.items():
        value = jnp.where(here == place, entry, value)
    return value


def packed(fields, base):
    return sum(field * base**i for i, field in enumerate(fields))


def kernel(
    n,
    q_hbm,
    k_hbm,
    v_hbm,
    out,
    q,
    flat,
    kv,
    acc,
    total,
    top,
    q_sem,
    loc_sem,
    halo_sem,
    send_sem,
    recv_sem,
):
    me = lax.axis_index("seq")
    tokens = q_hbm.shape[0]
    heads = q_hbm.shape[1] // HEAD_SIZE
    group = heads // KEY_VALUE_HEADS
    factor = math.log2(math.e) / math.sqrt(HEAD_SIZE)
    every = tuple(range(KEY_VALUE_HEADS))
    rows = group * tokens

    before = tokens + HALO
    anchor = pl.ds(0, tokens)
    halo = pl.ds(tokens, HALO)
    own = pl.ds(before, tokens)

    for h in every:
        columns = pl.ds(h * HEAD_SIZE, HEAD_SIZE)
        for side, ref in enumerate((k_hbm, v_hbm)):
            pltpu.make_async_copy(
                ref.at[:, columns], kv.at[h, side, own], loc_sem
            ).start()
    query_copy = pltpu.make_async_copy(q_hbm, q, q_sem)
    query_copy.start()

    block, trees, turns, late_halo = plan(n)
    here = me % block
    origin = me - here
    base = block + 1
    above = {d: set() for d in range(block)}
    for tree in trees:
        for d, below in tree.items():
            for child in below:
                above[child].add(d)
    for d in range(1, block):
        above[d].add(d - 1)
    ready_table = {
        d: sum(d in others for others in above.values()) for d in range(block)
    }

    barrier = pltpu.get_barrier_semaphore()
    most = max(len(others) for others in above.values())
    parents = pick(
        here, {d: packed([p + 1 for p in sorted(o)], base) for d, o in above.items()}
    )
    for i in range(most):
        parent = (parents // base**i) % base

        @pl.when(parent > 0)
        def _(parent=parent):
            pl.semaphore_signal(
                barrier,
                inc=1,
                device_id=(origin + parent - 1,),
                device_id_type=MESH,
            )

    ready = pick(here, ready_table)
    if n > block:
        @pl.when((here == 0) & (me > 0))
        def _():
            for target in (me - block, me - 1):
                pl.semaphore_signal(
                    barrier, inc=1, device_id=(target,), device_id_type=MESH
                )

        across = jnp.where((here == 0) | (here == block - 1), 1, 0)
        ready = ready + jnp.where(me + block < n, across, 0)
        ready = ready + jnp.where(
            (here == block - 1) & (me + block >= n) & (me < n - 1), 1, 0
        )

    slots = max(len(below) for tree in trees for below in tree.values())
    children = []
    for tree in trees:
        code = pick(
            here, {d: packed([c + 1 for c in below], base) for d, below in tree.items()}
        )
        targets = []
        for i in range(slots):
            child = (code // base**i) % base
            targets.append((child > 0, origin + child - 1))
        if n > block:
            targets.append(((here == 0) & (me + block < n), me + block))
        children.append(targets)
    turn = pick(here, turns)
    late = pick(here, late_halo)
    if n > block:
        turn = jnp.where((here == 0) & (me > 0), 0, turn)

    size = tokens // PARTS

    def to_child(start, h, slot, side, part):
        return pltpu.make_async_remote_copy(
            src_ref=kv.at[h, side, pl.ds(start + part * size, size)],
            dst_ref=kv.at[h, side, pl.ds(part * size, size)],
            send_sem=send_sem.at[slot, side],
            recv_sem=recv_sem.at[h, side, part],
            device_id=(children[side][slot][1],),
            device_id_type=MESH,
        )

    def forward(start, h, side, part):
        for slot, (condition, _) in enumerate(children[side]):

            @pl.when(condition)
            def _(slot=slot):
                to_child(start, h, slot, side, part).start()

    query_copy.wait()
    for i in range(heads):
        flat[:, i * tokens : (i + 1) * tokens] = q[
            :, i * HEAD_SIZE : (i + 1) * HEAD_SIZE
        ].T

    @pl.when(ready > 0)
    def _():
        pl.semaphore_wait(barrier, ready)

    pltpu.make_async_copy(kv.at[:, :, own], kv.at[:, :, own], loc_sem).wait()

    halo_copy = pltpu.make_async_remote_copy(
        src_ref=kv.at[:, :, pl.ds(before + tokens - HALO, HALO)],
        dst_ref=kv.at[:, :, halo],
        send_sem=halo_sem.at[0],
        recv_sem=halo_sem.at[1],
        device_id=((me + 1) % n,),
        device_id_type=MESH,
    )

    def send_halo(which):
        @pl.when((me < n - 1) & (late == which))
        def _():
            halo_copy.start()

    send_halo(0)

    @pl.when(me == 0)
    def _():
        for h in every:
            for side in range(2):
                for part in range(PARTS):
                    forward(before, h, side, part)

    def pass_on(h):
        for side in range(2):
            for part in range(PARTS):
                piece = kv.at[h, side, pl.ds(part * size, size)]
                pltpu.make_async_remote_copy(
                    src_ref=piece,
                    dst_ref=piece,
                    send_sem=send_sem.at[0, side],
                    recv_sem=recv_sem.at[h, side, part],
                    device_id=((me + 1) % n,),
                    device_id_type=MESH,
                ).wait_recv()
                forward(0, h, side, part)

    def pass_all():
        for h in every:
            pass_on(h)

    def scores(h, first, stop):
        return jnp.dot(
            kv[h, 0, first:stop],
            flat[:, h * rows : (h + 1) * rows],
            preferred_element_type=jnp.float32,
        )

    def weigh(s, highest):
        return jnp.exp2((s - highest) * factor).astype(jnp.bfloat16)

    def mix(h, first, stop, weights):
        value = kv[h, 1, first:stop]
        ones = jnp.ones((2 * SUM_ROWS, stop - first), value.dtype)
        both = jnp.dot(
            jnp.concatenate([value.T, ones], axis=0),
            weights,
            preferred_element_type=jnp.float32,
        )
        return both[:HEAD_SIZE], both[HEAD_SIZE : HEAD_SIZE + SUM_ROWS]

    def put(h, mixed, summed):
        first = h * group
        result = (mixed * (1.0 / summed[:1])).astype(out.dtype)
        for i in range(group):
            out[:, (first + i) * HEAD_SIZE : (first + i + 1) * HEAD_SIZE] = result[
                :, i * tokens : (i + 1) * tokens
            ].T

    def keep(h, mixed, summed, highest):
        acc[h] = mixed
        total[h] = summed
        top[h] = jnp.broadcast_to(highest, (SUM_ROWS, rows))

    def merged(h, first, stop):
        s = scores(h, first, stop)
        was = top[h]
        highest = jnp.maximum(was, jnp.max(s, axis=0, keepdims=True))
        drop = jnp.exp2((was - highest) * factor)
        mixed, summed = mix(h, first, stop, weigh(s, highest[:1]))
        mixed = mixed + acc[h] * drop[:1]
        summed = summed + total[h] * drop
        return mixed, summed, highest

    key_ids = lax.broadcasted_iota(jnp.int32, (tokens, rows), 0)
    query_ids = lax.broadcasted_iota(jnp.int32, (tokens, rows), 1) % tokens
    visible = key_ids <= query_ids

    @pl.when(turn == 0)
    def _():
        pass_all()
        send_halo(3)
        halo_copy.wait_recv()
        for h in every:
            s = scores(h, 0, before + tokens)
            others, mine = s[:before], jnp.where(visible, s[before:], -1e30)
            highest = jnp.maximum(
                jnp.max(others, axis=0, keepdims=True),
                jnp.max(mine, axis=0, keepdims=True),
            )
            weights = jnp.concatenate(
                [weigh(others, highest), weigh(mine, highest)], axis=0
            )
            put(h, *mix(h, 0, before + tokens, weights))

    @pl.when(turn > 0)
    def _():
        for h in every:
            s = jnp.where(visible, scores(h, before, before + tokens), -1e30)
            highest = jnp.max(s, axis=0, keepdims=True)
            mixed, summed = mix(h, before, before + tokens, weigh(s, highest))
            keep(h, mixed, summed, highest)

    @pl.when(me == 0)
    def _():
        for h in every:
            put(h, acc[h], total[h])

    send_halo(1)

    @pl.when(turn == 1)
    def _():
        pass_all()
        send_halo(2)

    @pl.when((turn == 1) | (turn == 4))
    def _():
        halo_copy.wait_recv()
        for h in every:

            @pl.when(turn == 4)
            def _(h=h):
                pass_on(h)

            mixed, summed, _ = merged(h, 0, before)
            put(h, mixed, summed)

    @pl.when((turn == 2) | (turn == 3))
    def _():
        halo_copy.wait_recv()
        for h in every:
            keep(h, *merged(h, tokens, before))
        send_halo(4)

        @pl.when(turn == 2)
        def _():
            pass_all()

        for h in every:

            @pl.when(turn == 3)
            def _(h=h):
                pass_on(h)

            mixed, summed, _ = merged(h, 0, tokens)
            put(h, mixed, summed)

    for side in range(2):
        for slot, (condition, _) in enumerate(children[side]):

            @pl.when(condition)
            def _(slot=slot, side=side):
                sent = kv.at[:, side, anchor]
                pltpu.make_async_remote_copy(
                    src_ref=sent,
                    dst_ref=sent,
                    send_sem=send_sem.at[slot, side],
                    recv_sem=recv_sem.at[0, side, 0],
                    device_id=(children[side][slot][1],),
                    device_id_type=MESH,
                ).wait_send()

    @pl.when(me < n - 1)
    def _():
        halo_copy.wait_send()


def attention(n, queries, keys, values):
    tokens, width = queries.shape
    rows = width // HEAD_SIZE // KEY_VALUE_HEADS * tokens
    block, trees, *_ = plan(n)
    slots = max(len(below) for tree in trees for below in tree.values()) + (n > block)
    state = pltpu.VMEM((KEY_VALUE_HEADS, HEAD_SIZE, rows), jnp.float32)
    row = pltpu.VMEM((KEY_VALUE_HEADS, SUM_ROWS, rows), jnp.float32)
    pieces = (KEY_VALUE_HEADS, 2, 2 * tokens + HALO, HEAD_SIZE)
    return pl.pallas_call(
        functools.partial(kernel, n),
        out_shape=pltpu.VMEM(queries.shape, queries.dtype),
        in_specs=[pl.BlockSpec(memory_space=pltpu.HBM)] * 3,
        out_specs=pl.BlockSpec(memory_space=pltpu.VMEM),
        scratch_shapes=[
            pltpu.VMEM(queries.shape, queries.dtype),
            pltpu.VMEM((HEAD_SIZE, KEY_VALUE_HEADS * rows), queries.dtype),
            pltpu.VMEM(pieces, keys.dtype),
            state,
            row,
            row,
            pltpu.SemaphoreType.DMA,
            pltpu.SemaphoreType.DMA,
            pltpu.SemaphoreType.DMA((2,)),
            pltpu.SemaphoreType.DMA((slots, 2)),
            pltpu.SemaphoreType.DMA((KEY_VALUE_HEADS, 2, PARTS)),
        ],
        compiler_params=pltpu.CompilerParams(
            collective_id=0, has_side_effects=True, vmem_limit_bytes=60 * 2**20
        ),
    )(queries, keys, values)


def solution(mesh):
    n = mesh.shape["seq"]
    return jax.shard_map(
        functools.partial(attention, n),
        mesh=mesh,
        in_specs=(P("seq", None), P("seq", None), P("seq", None)),
        out_specs=P("seq", None),
        check_vma=False,
    )
```

```python
import functools
import math

import jax
import jax.numpy as jnp
from jax import lax
from jax.experimental import pallas as pl
from jax.experimental.pallas import tpu as pltpu
from jax.sharding import PartitionSpec as P

KEY_VALUE_HEADS = 4
HEAD_SIZE = 128
HALO = 64
SUM_ROWS = 8
PARTS = 2
MESH = pl.DeviceIdType.MESH

BLOCK = 32
KEY_CHILDREN = {
    0: (9, 5, 3, 1,),
    3: (27, 7, 2,),
    5: (29, 4,),
    7: (23, 6,),
    9: (11, 8, 13, 17,),
    11: (10, 15,),
    13: (12,),
    15: (14,),
    17: (21, 19, 25, 16,),
    19: (18,),
    21: (20,),
    23: (22,),
    25: (24,),
    27: (26, 31,),
    29: (28,),
    31: (30,),
}
VALUE_CHILDREN = {
    0: (5, 3, 9, 1,),
    3: (27, 7, 2,),
    5: (29, 4,),
    7: (23, 6,),
    9: (11, 17, 13, 8,),
    11: (15, 10,),
    13: (12,),
    15: (14,),
    17: (21, 19, 25, 16,),
    19: (18,),
    21: (20,),
    23: (22,),
    25: (24,),
    27: (26, 31,),
    29: (28,),
    31: (30,),
}
TURN = {0: 5, 1: 3, 2: 1, 3: 0, 4: 4, 5: 1, 6: 3, 7: 4, 8: 4, 9: 0, 10: 3, 11: 2, 12: 3, 13: 3, 14: 3, 15: 3, 16: 4, 17: 0, 18: 3, 19: 3, 20: 3, 21: 3, 22: 3, 23: 3, 24: 3, 25: 3, 26: 4, 27: 1, 28: 4, 29: 4, 30: 3, 31: 3}
LATE_HALO = {1: 4, 4: 1, 8: 1, 15: 1, 16: 1, 20: 1, 24: 1, 25: 1, 26: 1, 27: 1, 29: 1}


def plan(n):
    if n % BLOCK == 0:
        return BLOCK, (KEY_CHILDREN, VALUE_CHILDREN), TURN, LATE_HALO
    chain = {d: (d + 1,) for d in range(n - 1)}
    return n, (chain, chain), {d: 3 if d else 5 for d in range(n)}, {}


def pick(here, table):
    value = 0
    for place, entry in table.items():
        value = jnp.where(here == place, entry, value)
    return value


def packed(fields, base):
    return sum(field * base**i for i, field in enumerate(fields))


def kernel(
    n,
    q_hbm,
    k_hbm,
    v_hbm,
    out,
    q,
    flat,
    kv,
    acc,
    total,
    top,
    q_sem,
    loc_sem,
    halo_sem,
    send_sem,
    recv_sem,
):
    me = lax.axis_index("seq")
    tokens = q_hbm.shape[0]
    heads = q_hbm.shape[1] // HEAD_SIZE
    group = heads // KEY_VALUE_HEADS
    factor = math.log2(math.e) / math.sqrt(HEAD_SIZE)
    every = tuple(range(KEY_VALUE_HEADS))
    rows = group * tokens

    before = tokens + HALO
    anchor = pl.ds(0, tokens)
    halo = pl.ds(tokens, HALO)
    own = pl.ds(before, tokens)

    for h in every:
        columns = pl.ds(h * HEAD_SIZE, HEAD_SIZE)
        for side, ref in enumerate((k_hbm, v_hbm)):
            pltpu.make_async_copy(
                ref.at[:, columns], kv.at[h, side, own], loc_sem
            ).start()
    query_copy = pltpu.make_async_copy(q_hbm, q, q_sem)
    query_copy.start()

    block, trees, turns, late_halo = plan(n)
    here = me % block
    origin = me - here
    base = block + 1
    above = {d: set() for d in range(block)}
    for tree in trees:
        for d, below in tree.items():
            for child in below:
                above[child].add(d)
    for d in range(1, block):
        above[d].add(d - 1)
    ready_table = {
        d: sum(d in others for others in above.values()) for d in range(block)
    }

    barrier = pltpu.get_barrier_semaphore()
    most = max(len(others) for others in above.values())
    parents = pick(
        here, {d: packed([p + 1 for p in sorted(o)], base) for d, o in above.items()}
    )
    for i in range(most):
        parent = (parents // base**i) % base

        @pl.when(parent > 0)
        def _(parent=parent):
            pl.semaphore_signal(
                barrier,
                inc=1,
                device_id=(origin + parent - 1,),
                device_id_type=MESH,
            )

    ready = pick(here, ready_table)
    if n > block:
        @pl.when((here == 0) & (me > 0))
        def _():
            for target in (me - block, me - 1):
                pl.semaphore_signal(
                    barrier, inc=1, device_id=(target,), device_id_type=MESH
                )

        across = jnp.where((here == 0) | (here == block - 1), 1, 0)
        ready = ready + jnp.where(me + block < n, across, 0)
        ready = ready + jnp.where(
            (here == block - 1) & (me + block >= n) & (me < n - 1), 1, 0
        )

    slots = max(len(below) for tree in trees for below in tree.values())
    children = []
    for tree in trees:
        code = pick(
            here, {d: packed([c + 1 for c in below], base) for d, below in tree.items()}
        )
        targets = []
        for i in range(slots):
            child = (code // base**i) % base
            targets.append((child > 0, origin + child - 1))
        if n > block:
            targets.append(((here == 0) & (me + block < n), me + block))
        children.append(targets)
    turn = pick(here, turns)
    late = pick(here, late_halo)
    if n > block:
        turn = jnp.where((here == 0) & (me > 0), 0, turn)

    size = tokens // PARTS

    def to_child(start, h, slot, side, part):
        return pltpu.make_async_remote_copy(
            src_ref=kv.at[h, side, pl.ds(start + part * size, size)],
            dst_ref=kv.at[h, side, pl.ds(part * size, size)],
            send_sem=send_sem.at[slot, side],
            recv_sem=recv_sem.at[h, side, part],
            device_id=(children[side][slot][1],),
            device_id_type=MESH,
        )

    def forward(start, h, side, part):
        for slot, (condition, _) in enumerate(children[side]):

            @pl.when(condition)
            def _(slot=slot):
                to_child(start, h, slot, side, part).start()

    query_copy.wait()
    for i in range(heads):
        flat[:, i * tokens : (i + 1) * tokens] = q[
            :, i * HEAD_SIZE : (i + 1) * HEAD_SIZE
        ].T

    @pl.when(ready > 0)
    def _():
        pl.semaphore_wait(barrier, ready)

    pltpu.make_async_copy(kv.at[:, :, own], kv.at[:, :, own], loc_sem).wait()

    halo_copy = pltpu.make_async_remote_copy(
        src_ref=kv.at[:, :, pl.ds(before + tokens - HALO, HALO)],
        dst_ref=kv.at[:, :, halo],
        send_sem=halo_sem.at[0],
        recv_sem=halo_sem.at[1],
        device_id=((me + 1) % n,),
        device_id_type=MESH,
    )

    def send_halo(which):
        @pl.when((me < n - 1) & (late == which))
        def _():
            halo_copy.start()

    send_halo(0)

    @pl.when(me == 0)
    def _():
        for h in every:
            for side in range(2):
                for part in range(PARTS):
                    forward(before, h, side, part)

    def pass_on(h):
        for side in range(2):
            for part in range(PARTS):
                piece = kv.at[h, side, pl.ds(part * size, size)]
                pltpu.make_async_remote_copy(
                    src_ref=piece,
                    dst_ref=piece,
                    send_sem=send_sem.at[0, side],
                    recv_sem=recv_sem.at[h, side, part],
                    device_id=((me + 1) % n,),
                    device_id_type=MESH,
                ).wait_recv()
                forward(0, h, side, part)

    def pass_all():
        for h in every:
            pass_on(h)

    def scores(h, first, stop):
        return jnp.dot(
            kv[h, 0, first:stop],
            flat[:, h * rows : (h + 1) * rows],
            preferred_element_type=jnp.float32,
        )

    def weigh(s, highest):
        return jnp.exp2((s - highest) * factor).astype(jnp.bfloat16)

    def mix(h, first, stop, weights):
        value = kv[h, 1, first:stop]
        ones = jnp.ones((2 * SUM_ROWS, stop - first), value.dtype)
        both = jnp.dot(
            jnp.concatenate([value.T, ones], axis=0),
            weights,
            preferred_element_type=jnp.float32,
        )
        return both[:HEAD_SIZE], both[HEAD_SIZE : HEAD_SIZE + SUM_ROWS]

    def put(h, mixed, summed):
        first = h * group
        result = (mixed * (1.0 / summed[:1])).astype(out.dtype)
        for i in range(group):
            out[:, (first + i) * HEAD_SIZE : (first + i + 1) * HEAD_SIZE] = result[
                :, i * tokens : (i + 1) * tokens
            ].T

    def keep(h, mixed, summed, highest):
        acc[h] = mixed
        total[h] = summed
        top[h] = jnp.broadcast_to(highest, (SUM_ROWS, rows))

    def merged(h, first, stop):
        s = scores(h, first, stop)
        was = top[h]
        highest = jnp.maximum(was, jnp.max(s, axis=0, keepdims=True))
        drop = jnp.exp2((was - highest) * factor)
        mixed, summed = mix(h, first, stop, weigh(s, highest[:1]))
        mixed = mixed + acc[h] * drop[:1]
        summed = summed + total[h] * drop
        return mixed, summed, highest

    key_ids = lax.broadcasted_iota(jnp.int32, (tokens, rows), 0)
    query_ids = lax.broadcasted_iota(jnp.int32, (tokens, rows), 1) % tokens
    visible = key_ids <= query_ids

    @pl.when(turn == 0)
    def _():
        pass_all()
        send_halo(3)
        halo_copy.wait_recv()
        for h in every:
            s = scores(h, 0, before + tokens)
            others, mine = s[:before], jnp.where(visible, s[before:], -1e30)
            highest = jnp.maximum(
                jnp.max(others, axis=0, keepdims=True),
                jnp.max(mine, axis=0, keepdims=True),
            )
            weights = jnp.concatenate(
                [weigh(others, highest), weigh(mine, highest)], axis=0
            )
            put(h, *mix(h, 0, before + tokens, weights))

    @pl.when(turn > 0)
    def _():
        for h in every:
            s = jnp.where(visible, scores(h, before, before + tokens), -1e30)
            highest = jnp.max(s, axis=0, keepdims=True)
            mixed, summed = mix(h, before, before + tokens, weigh(s, highest))
            keep(h, mixed, summed, highest)

    @pl.when(me == 0)
    def _():
        for h in every:
            put(h, acc[h], total[h])

    send_halo(1)

    @pl.when(turn == 1)
    def _():
        pass_all()
        send_halo(2)

    @pl.when((turn == 1) | (turn == 4))
    def _():
        halo_copy.wait_recv()
        for h in every:

            @pl.when(turn == 4)
            def _(h=h):
                pass_on(h)

            mixed, summed, _ = merged(h, 0, before)
            put(h, mixed, summed)

    @pl.when((turn == 2) | (turn == 3))
    def _():
        halo_copy.wait_recv()
        for h in every:
            keep(h, *merged(h, tokens, before))
        send_halo(4)

        @pl.when(turn == 2)
        def _():
            pass_all()

        for h in every:

            @pl.when(turn == 3)
            def _(h=h):
                pass_on(h)

            mixed, summed, _ = merged(h, 0, tokens)
            put(h, mixed, summed)

    for side in range(2):
        for slot, (condition, _) in enumerate(children[side]):

            @pl.when(condition)
            def _(slot=slot, side=side):
                sent = kv.at[:, side, anchor]
                pltpu.make_async_remote_copy(
                    src_ref=sent,
                    dst_ref=sent,
                    send_sem=send_sem.at[slot, side],
                    recv_sem=recv_sem.at[0, side, 0],
                    device_id=(children[side][slot][1],),
                    device_id_type=MESH,
                ).wait_send()

    @pl.when(me < n - 1)
    def _():
        halo_copy.wait_send()


def attention(n, queries, keys, values):
    tokens, width = queries.shape
    rows = width // HEAD_SIZE // KEY_VALUE_HEADS * tokens
    block, trees, *_ = plan(n)
    slots = max(len(below) for tree in trees for below in tree.values()) + (n > block)
    state = pltpu.VMEM((KEY_VALUE_HEADS, HEAD_SIZE, rows), jnp.float32)
    row = pltpu.VMEM((KEY_VALUE_HEADS, SUM_ROWS, rows), jnp.float32)
    pieces = (KEY_VALUE_HEADS, 2, 2 * tokens + HALO, HEAD_SIZE)
    return pl.pallas_call(
        functools.partial(kernel, n),
        out_shape=pltpu.VMEM(queries.shape, queries.dtype),
        in_specs=[pl.BlockSpec(memory_space=pltpu.HBM)] * 3,
        out_specs=pl.BlockSpec(memory_space=pltpu.VMEM),
        scratch_shapes=[
            pltpu.VMEM(queries.shape, queries.dtype),
            pltpu.VMEM((HEAD_SIZE, KEY_VALUE_HEADS * rows), queries.dtype),
            pltpu.VMEM(pieces, keys.dtype),
            state,
            row,
            row,
            pltpu.SemaphoreType.DMA,
            pltpu.SemaphoreType.DMA,
            pltpu.SemaphoreType.DMA((2,)),
            pltpu.SemaphoreType.DMA((slots, 2)),
            pltpu.SemaphoreType.DMA((KEY_VALUE_HEADS, 2, PARTS)),
        ],
        compiler_params=pltpu.CompilerParams(
            collective_id=0, has_side_effects=True, vmem_limit_bytes=60 * 2**20
        ),
    )(queries, keys, values)


def solution(mesh):
    n = mesh.shape["seq"]
    return jax.shard_map(
        functools.partial(attention, n),
        mesh=mesh,
        in_specs=(P("seq", None), P("seq", None), P("seq", None)),
        out_specs=P("seq", None),
        check_vma=False,
    )
```
